32 devices in a mesh: groups: 2 (over y), fsdp: 4 (over z), expert: 4 (over x, core).
Axes of the slice: x: 2, y: 2, z: 4, core: 2. Of those that a mesh axis runs over, the one named last changes fastest.
Arguments:
- queries: bfloat16 [512, 2048], P(('groups', 'fsdp'), 'expert'), parts along dimension 0, may hold values from -14 to 14
- keys: bfloat16 [8, 2048, 512], P(('groups', 'fsdp'), None, 'expert'), parts along dimension 0, may hold values from -14 to 14
- values: bfloat16 [8, 2048, 512], P(('groups', 'fsdp'), None, 'expert'), parts along dimension 0, may hold values from -4 to 4
- out_weight: bfloat16 [2048, 4096], P('expert', 'fsdp'), may hold values from -0.5 to 0.5
- residual: bfloat16 [512, 4096], P(('groups', 'fsdp')), parts along dimension 0, may hold values from -3 to 3
- norm_gain: float32 [4096], replicated, may hold values from 0.5 to 1.5
- route_ids: int32 [512, 2], P(('groups', 'fsdp')), parts along dimension 0, may hold values from 0 to 7, as said below
- route_slots: int32 [512, 2], P(('groups', 'fsdp')), parts along dimension 0, may hold values from 0 to 23, as said below
- route_weights: int32 [512, 2], P(('groups', 'fsdp')), parts along dimension 0, may hold values from 1 to 65535, as said below
- w_gate: bfloat16 [8, 4096, 7168], P('expert', None, 'fsdp'), may hold values from -0.09375 to 0.09375
- w_up: bfloat16 [8, 4096, 7168], P('expert', None, 'fsdp'), may hold values from -0.09375 to 0.09375
- w_down: bfloat16 [8, 7168, 4096], P('expert', 'fsdp'), may hold values from -0.0625 to 0.0625
Outputs:
- layer_out: bfloat16 [512, 4096], P(('groups', 'fsdp'), 'expert'), parts along dimension 0
The draws below stay inside these ranges and needn't reach their ends.
There are 2 independent parts, one for each index of `groups`. The reference program is written for one: setup_inputs(seed, part) draws one part's arguments, and reference() takes and returns one part's arrays. A program takes and returns all parts, laid end to end along the dimension named above; an argument that names none is the same for every part. Nothing has to cross between parts.
Inputs may be any that keep to these rules, and one draw needn't show every extreme that they name: `route_ids`: each row names two different experts. Among the rows of one block, no expert is named more than 24 times and no group of experts 2 g and 2 g + 1 more than 36 times; one expert, the same for all blocks, is named exactly 24 times in every block and its group exactly 36 times; every expert is named in every block. `route_slots`: within one block, the routes to one expert hold the slots 0 to their count - 1, each once. `route_weights`: the two entries of a row sum to 65536.
All inputs are finite; a program needn't handle non-finite values.
Results may differ from the reference program's by a relative error of at most 0.02.
Values may be sent and summed in bfloat16 or wider, within the bound.
A program may use at most 192 MiB of HBM per device.

```python
import jax
import jax.numpy as jnp
from jax import lax

D = 4096
HEADS = 16
KV_HEADS = 4
HEAD_DIM = 128
EXPERTS = 8
FFW = 7168
Q_BLOCK = 64
CTX = 2048
CAP = 24
GCAP = 36
SEQS = 4
TOKENS = 256
N_FSDP = 4


def draw_queries(key, part):
    base_key = jax.random.fold_in(key, 5)
    shape = (SEQS, Q_BLOCK, KV_HEADS, HEADS // KV_HEADS, HEAD_DIM)
    base = jnp.clip(1.5 * jax.random.normal(base_key, shape, jnp.float32), -6.0, 6.0)
    return base.reshape(TOKENS, HEADS * HEAD_DIM).astype(jnp.bfloat16)


def draw_keys(key, part):
    base_key = jax.random.fold_in(key, 6)
    shape = (SEQS, CTX, KV_HEADS, HEAD_DIM)
    base = jnp.clip(jax.random.normal(base_key, shape, jnp.float32), -4.0, 4.0)
    return base.reshape(SEQS, CTX, KV_HEADS * HEAD_DIM).astype(jnp.bfloat16)


def shuffle_one(key):
    return jax.random.permutation(key, Q_BLOCK)


def route_table(key):
    sub = jax.random.fold_in(key, 11)
    busy_key, sum_key, turn_key, split_key, order_key = jax.random.split(sub, 5)
    busy = jax.random.randint(busy_key, (), 0, EXPERTS)
    busy_pair = busy // 2
    lower = 7 * Q_BLOCK // 16
    drawn = jax.random.randint(sum_key, (SEQS, 2), lower, GCAP + 1)
    third = 2 * Q_BLOCK - GCAP - drawn[:, 0] - drawn[:, 1]
    others = jnp.concatenate([drawn, third[:, None]], axis=1)
    turn = jax.random.randint(turn_key, (SEQS, 1), 0, 3)
    others = jnp.take_along_axis(others, (jnp.arange(3)[None, :] + turn) % 3, axis=1)
    pairs = jnp.arange(EXPERTS // 2)
    other_index = jnp.clip(pairs - (pairs > busy_pair).astype(jnp.int32), 0, 2)
    pair_sums = jnp.where(pairs[None, :] == busy_pair, GCAP, jnp.take(others, other_index, axis=1))
    low_split = jnp.maximum(pair_sums - CAP, 1)
    high_split = jnp.minimum(pair_sums - 1, CAP)
    evens = jax.random.randint(split_key, (SEQS, EXPERTS // 2), low_split, high_split + 1)
    busy_even = jnp.where(busy % 2 == 0, CAP, GCAP - CAP)
    evens = jnp.where(pairs[None, :] == busy_pair, busy_even, evens)
    counts = jnp.stack([evens, pair_sums - evens], axis=2).reshape(SEQS, EXPERTS)
    ends = jnp.cumsum(counts, axis=1)
    starts = ends - counts
    position = jnp.arange(2 * Q_BLOCK)
    owner = jnp.sum((ends[:, None, :] <= position[None, :, None]).astype(jnp.int32), axis=2)
    rank = position[None, :] - jnp.take_along_axis(starts, owner, axis=1)
    order = jax.vmap(shuffle_one)(jax.random.split(order_key, SEQS))
    pick = jnp.stack([order, order + Q_BLOCK], axis=2).reshape(SEQS, 2 * Q_BLOCK)
    route_ids = jnp.take_along_axis(owner, pick, axis=1).reshape(TOKENS, 2)
    route_slots = jnp.take_along_axis(rank, pick, axis=1).reshape(TOKENS, 2)
    return (route_ids.astype(jnp.int32), route_slots.astype(jnp.int32))


def draw_route_ids(key, part):
    return route_table(key)[0]


def draw_route_slots(key, part):
    return route_table(key)[1]


def draw_route_weights(key, part):
    leading = jax.random.randint(jax.random.fold_in(key, 3), (TOKENS,), 1, 65536)
    return jnp.stack([leading, 65536 - leading], axis=1).astype(jnp.int32)


def levels(stream_key, shape, shards, least, top_value):
    loudness, own = 1.0, jax.random.fold_in(stream_key, 6)
    for axis_at, parts in shards:
        heights = jnp.exp(jax.random.uniform(jax.random.fold_in(own, axis_at), (parts,), jnp.float32, least / len(shards), top_value / len(shards)))
        loudness = loudness * jnp.repeat(heights, shape[axis_at] // parts).reshape([-1 if axis == axis_at else 1 for axis in range(len(shape))])
    return loudness


def normal_values(rng, extent, scale, bound, pieces=(), kind=jnp.bfloat16):
    factor_of = levels(rng, extent, pieces, -0.22, 0.18) if pieces else 1.0
    entries = jax.random.normal(rng, extent, jnp.float32) * scale * factor_of
    return jnp.minimum(jnp.maximum(entries, -bound), bound).astype(kind)


def setup_inputs(seed: int = 0, part: int = 0) -> dict:
    key_list = jax.random.split(jax.random.key(seed), 13)
    part_keys = jax.random.split(jax.random.fold_in(key_list[12], part), 13)
    return {
        "queries": draw_queries(jax.random.fold_in(jax.random.fold_in(key_list[12], part), 71), part),
        "keys": draw_keys(jax.random.fold_in(jax.random.fold_in(key_list[12], part), 71), part),
        "values": normal_values(part_keys[2], (SEQS, CTX, KV_HEADS * HEAD_DIM), 1.0, 4.0, ((0, 4), (2, 4))),
        "out_weight": normal_values(key_list[3], (HEADS * HEAD_DIM, D), HEAD_DIM ** -0.5, 0.5, ((0, 4), (1, 4))),
        "residual": normal_values(part_keys[4], (TOKENS, D), 0.5, 3.0, ((0, 4),)),
        "norm_gain": jnp.clip(1.0 + 0.1 * jax.random.normal(key_list[5], (D,), jnp.float32), 0.5, 1.5),
        "route_ids": draw_route_ids(jax.random.fold_in(jax.random.fold_in(key_list[12], part), 71), part),
        "route_slots": draw_route_slots(jax.random.fold_in(jax.random.fold_in(key_list[12], part), 71), part),
        "route_weights": draw_route_weights(jax.random.fold_in(jax.random.fold_in(key_list[12], part), 71), part),
        "w_gate": normal_values(key_list[9], (EXPERTS, D, FFW), D ** -0.5, 0.09375, ((0, 4), (2, 4))),
        "w_up": normal_values(key_list[10], (EXPERTS, D, FFW), D ** -0.5, 0.09375, ((0, 4), (2, 4))),
        "w_down": normal_values(key_list[11], (EXPERTS, FFW, D), FFW ** -0.5, 0.0625, ((0, 4), (1, 4))),
    }


eps = 1e-05

def attend_one(item):
    query_block, key_block, value_block = item
    block = query_block.shape[0]
    context = key_block.shape[0]
    group = HEADS // KV_HEADS
    query_heads = query_block.reshape(block, KV_HEADS, group, HEAD_DIM).astype(jnp.float32)
    key_heads = key_block.reshape(context, KV_HEADS, HEAD_DIM).astype(jnp.float32)
    value_heads = value_block.reshape(context, KV_HEADS, HEAD_DIM).astype(jnp.float32)
    scores = jnp.einsum('qcgd,kcd->cgqk', query_heads, key_heads) * HEAD_DIM ** (-0.5)
    key_pos = jnp.arange(context)
    query_pos = context - block + jnp.arange(block)
    allowed = key_pos[None, :] <= query_pos[:, None]
    masked = jnp.where(allowed, scores, -1e+30)
    highest = lax.optimization_barrier(jnp.max(masked, axis=-1, keepdims=True))
    weights = jnp.where(allowed, jnp.exp(masked - highest), 0.0)
    probs = (weights / lax.optimization_barrier(jnp.sum(weights, axis=-1, keepdims=True))).astype(jnp.bfloat16)
    heads_out = jnp.einsum('cgqk,kcd->qcgd', probs.astype(jnp.float32), value_heads)
    return heads_out.astype(jnp.bfloat16).reshape(block, HEADS * HEAD_DIM)

def expert_one(item):
    rows, gate_w, up_w, down_w = item
    gate = jnp.dot(rows, gate_w, preferred_element_type=jnp.float32)
    upper = jnp.dot(rows, up_w, preferred_element_type=jnp.float32)
    hidden = (jax.nn.silu(gate) * upper).astype(jnp.bfloat16)
    width = FFW // N_FSDP
    hidden_runs = hidden.reshape(rows.shape[0], N_FSDP, width).transpose(1, 0, 2)
    down_runs = down_w.reshape(N_FSDP, width, down_w.shape[1])

    def add_run(total, pair):
        part = jnp.dot(pair[0], pair[1], preferred_element_type=jnp.float32)
        part = lax.optimization_barrier(part.astype(jnp.bfloat16)).astype(jnp.float32)
        return (total + part, None)
    start_total = jnp.zeros((rows.shape[0], down_w.shape[1]), jnp.float32)
    total, unused = lax.scan(add_run, start_total, (hidden_runs, down_runs))
    return total

def reference(queries, keys, values, out_weight, residual, norm_gain, route_ids, route_slots, route_weights, w_gate, w_up, w_down):
    query_blocks = queries.reshape(SEQS, Q_BLOCK, HEADS * HEAD_DIM)
    heads_out = lax.map(attend_one, (query_blocks, keys, values)).reshape(TOKENS, HEADS * HEAD_DIM)
    attn = jnp.dot(heads_out, out_weight, preferred_element_type=jnp.float32)
    hstate = (residual.astype(jnp.float32) + attn).astype(jnp.bfloat16)
    state = hstate.astype(jnp.float32)
    scale = lax.rsqrt(lax.optimization_barrier(jnp.mean(state * state, axis=-1, keepdims=True)) + eps)
    normed = (state * scale * norm_gain).astype(jnp.bfloat16)
    block_of = (jnp.arange(TOKENS) // Q_BLOCK).astype(jnp.int32)
    spread = jnp.broadcast_to(normed[:, None, :], (TOKENS, 2, D))
    buffer = jnp.zeros((SEQS, EXPERTS, CAP, D), jnp.bfloat16)
    buffer = buffer.at[block_of[:, None], route_ids, route_slots].set(spread)
    expert_rows = buffer.transpose(1, 0, 2, 3).reshape(EXPERTS, SEQS * CAP, D)
    expert_out = lax.map(expert_one, (expert_rows, w_gate, w_up, w_down)).reshape(EXPERTS, SEQS, CAP, D)
    picked = expert_out[route_ids, block_of[:, None], route_slots]
    route_share = route_weights.astype(jnp.float32) / 65536.0
    moe = lax.optimization_barrier(jnp.sum(route_share[:, :, None] * picked, axis=1))
    return (hstate.astype(jnp.float32) + moe).astype(jnp.bfloat16)
```

```python
import functools

import jax
import jax.numpy as jnp
from jax import lax
from jax.experimental import pallas as pl
from jax.experimental.pallas import tpu as pltpu
from jax.sharding import PartitionSpec as P

HEAD_DIM = 128
CAP = 24
EPS = 1e-05
MESH = pl.DeviceIdType.MESH
F32 = jnp.float32
BF16 = jnp.bfloat16
HALVES = 2
D_SLOTS = 4


def loop(low, high, body):
    if high - low <= 8:
        for i in range(low, high):
            body(i)
    else:
        lax.fori_loop(low, high, lambda i, c: (body(i), c)[1], 0)


def when(cond, body):
    if isinstance(cond, bool):
        if cond:
            body()
    else:
        pl.when(cond)(body)


def kernel(
    F, G,
    q_hbm, k_hbm, v_hbm, ow_hbm, res_hbm, gain_ref, ids_ref, slots_ref, wts_ref, wg_ref, wu_ref, wd_ref,
    out_ref,
    q_ref, k_ref, v_ref, ow_ref, res_ref,
    heads, routes, res_in, part, rs_in, attn_own, h_all, oh, lhs, ssq, acc, hid, ybuf,
    cbuf, a_in, b_in, c_in, wslot, dslot,
    in_sem, hs_s, hs_r, rt_s, rt_r, re_s, re_r, rs_s, rs_r, hz_s, hz_r, hx_s, hx_r, hc_s, hc_r,
    a_s, a_r, b_s, b_r, c_s, c_r, w_sem, d_sem,
):
    f = lax.axis_index("fsdp")
    g = lax.axis_index("expert")
    FG = F // G
    Q = q_ref.shape[0]
    ctx = k_ref.shape[0]
    C = ow_ref.shape[1]
    D = wg_ref.shape[1]
    C2 = D // G
    CH = C2 // HALVES
    n_heads = q_ref.shape[1] // HEAD_DIM

    def flip(a, m, n):
        if isinstance(m, int) and m == 0:
            return a
        out = 0
        bit = 1
        while bit < n:
            low = lax.rem(lax.div(a, bit), 2)
            if isinstance(m, int):
                mine = (m // bit) % 2
                low = 1 - low if mine else low
            else:
                mine = lax.rem(lax.div(m, bit), 2)
                low = low + mine - 2 * low * mine
            out = out + bit * low
            bit *= 2
        return out

    def peer(i):
        if F & (F - 1) == 0:
            return flip(f, i, F)
        return lax.rem(f + i, F)

    def copy(src, dst, s, r, **dev):
        return pltpu.make_async_remote_copy(
            src_ref=src, dst_ref=dst, send_sem=s, recv_sem=r,
            device_id=dev, device_id_type=MESH,
        )

    barrier = pltpu.get_barrier_semaphore()

    def greet_f(i):
        pl.semaphore_signal(barrier, inc=1, device_id={"fsdp": lax.rem(f + i, F)}, device_id_type=MESH)

    loop(1, F, greet_f)
    for i in range(1, G):
        pl.semaphore_signal(
            barrier, inc=1, device_id={"expert": lax.rem(g + i, G)}, device_id_type=MESH)

    loads = [
        pltpu.make_async_copy(src, dst, in_sem.at[i])
        for i, (src, dst) in enumerate((
            (q_hbm, q_ref), (k_hbm, k_ref), (v_hbm, v_ref), (res_hbm, res_ref), (ow_hbm, ow_ref)))
    ]
    for c in loads:
        c.start()

    def w_copies(k):
        col = peer(k)
        rows = pl.ds(pl.multiple_of(col * C, C), C)
        two = k % 2
        out = []
        for e in range(2):
            for t, ref in enumerate((wg_ref, wu_ref)):
                out.append(pltpu.make_async_copy(
                    ref.at[e, rows, :], wslot.at[two, 2 * e + t], w_sem.at[two, 2 * e + t]))
        return out

    masks = (3, 2, 1, 0)

    def d_copies(n):
        block = flip(g, masks[n % 4], G)
        cols = pl.ds(pl.multiple_of(block * C2 + (n // 4) * CH, CH), CH)
        return [
            pltpu.make_async_copy(wd_ref.at[e, :, cols], dslot.at[n % D_SLOTS, e], d_sem.at[n % D_SLOTS, e])
            for e in range(2)
        ]

    routes[f] = jnp.zeros((8, 128), jnp.int32)
    for t, ref in enumerate((ids_ref, slots_ref, wts_ref)):
        routes[f, 2 * t:2 * t + 2, :Q] = ref[...]

    n_kv = k_ref.shape[1] // HEAD_DIM
    per = n_heads // n_kv
    rate = HEAD_DIM ** (-0.5) * 1.4426950408889634
    for c in loads:
        c.wait()
    for k in range(min(2, F)):
        for c in w_copies(k):
            c.start()
    for n in range(D_SLOTS):
        for c in d_copies(n):
            c.start()

    for kv in range(n_kv):
        cols = slice(kv * HEAD_DIM, (kv + 1) * HEAD_DIM)
        qs = jnp.concatenate(
            [q_ref[:, h * HEAD_DIM:(h + 1) * HEAD_DIM] for h in range(kv * per, (kv + 1) * per)], axis=0)
        s = lax.dot_general(qs, k_ref[:, cols], (((1,), (1,)), ((), ())), preferred_element_type=F32)
        tail = 128
        key_pos = ctx - tail + lax.broadcasted_iota(jnp.int32, (per, Q, tail), 2)
        query_pos = ctx - Q + lax.broadcasted_iota(jnp.int32, (per, Q, tail), 1)
        allowed = (key_pos <= query_pos).reshape(per * Q, tail)
        s = jnp.concatenate([s[:, :ctx - tail], jnp.where(allowed, s[:, ctx - tail:], -1e30)], axis=1)
        top = jnp.max(s, axis=1, keepdims=True)
        w = jnp.exp2((s - top) * rate)
        total = jnp.sum(w, axis=1, keepdims=True)
        o = jnp.dot(w.astype(BF16), v_ref[:, cols], preferred_element_type=F32) / total
        for n in range(per):
            h = kv * per + n
            heads[f, :, h * HEAD_DIM:(h + 1) * HEAD_DIM] = o[n * Q:(n + 1) * Q].astype(BF16)

    pl.semaphore_wait(barrier, F - 1 + G - 1)

    def rt_copy(i):
        return copy(routes.at[f], routes.at[f], rt_s.at[i], rt_r.at[f], fsdp=peer(i))

    def rt_got(i):
        p = peer(i)
        return copy(routes.at[p], routes.at[p], rt_s.at[i], rt_r.at[p], fsdp=p)

    def cols_of(p):
        return pl.ds(pl.multiple_of(p * C, C), C)

    own_part = (f // FG) == g
    mine = f % FG

    def re_copy(i):
        p = peer(i)
        return copy(res_ref.at[:, cols_of(p)], res_in.at[mine], re_s.at[i], re_r.at[mine], fsdp=p)

    def hs_copy(i):
        return copy(heads.at[f], heads.at[f], hs_s.at[i], hs_r.at[f], fsdp=peer(i))

    def hs_got(p):
        return copy(heads.at[p], heads.at[p], hs_s.at[0], hs_r.at[p], fsdp=p)

    loop(1, F, lambda i: hs_copy(i).start())
    loop(1, F, lambda i: rt_copy(i).start())

    @pl.when(own_part)
    def _():
        loop(1, F, lambda i: re_copy(i).start())
        res_in[mine] = res_ref[:, cols_of(f)]

    ssq[...] = jnp.zeros_like(ssq)

    def rs_copy(j):
        return copy(part.at[j], rs_in.at[g], rs_s.at[j], rs_r.at[g], expert=j)

    def rs_got(e):
        return copy(part.at[e], rs_in.at[e], rs_s.at[e], rs_r.at[e], expert=e)

    def project(i):
        j = flip(f // FG, i, G)

        def arrive(n):
            p = j * FG + n

            @pl.when(p != f)
            def _():
                hs_got(p).wait_recv()

        loop(0, FG, arrive)
        rows = heads[pl.ds(j * FG, FG)].reshape(FG * Q, n_heads * HEAD_DIM)
        y = jnp.dot(rows, ow_ref[...], preferred_element_type=F32).reshape(FG, Q, C)

        @pl.when(j == g)
        def _():
            attn_own[...] = y

        @pl.when(j != g)
        def _():
            part[j] = y.astype(BF16)
            rs_copy(j).start()

    for i in range(G):
        project(i)

    loop(1, F, lambda i: rt_got(i).wait_recv())

    def tables(s):
        r = routes[s]
        slot_row = lax.broadcasted_iota(jnp.int32, (2 * CAP, Q), 0)
        table = jnp.zeros((2 * CAP, Q), F32)
        weight = jnp.zeros((2 * CAP, Q), F32)
        for t in range(2):
            within = r[t:t + 1, :Q] - 2 * g
            inside = (within >= 0) & (within < 2)
            row = jnp.where(inside, r[2 + t:3 + t, :Q] + CAP * within, -1)
            hit = (row == slot_row).astype(F32)
            table = table + hit
            weight = weight + hit * (r[4 + t:5 + t, :Q].astype(F32) / 65536.0)
        oh[s, :, :Q] = table
        oh[s, :, Q:] = jnp.broadcast_to(jnp.sum(weight, axis=1, keepdims=True), (2 * CAP, 128 - Q))

    loop(0, F, tables)

    far, near, both = flip(g, 2, G), flip(g, 1, G), flip(g, 3, G)

    def re_got(i):
        p = g * FG + i
        return copy(res_in.at[i], res_in.at[i], re_s.at[0], re_r.at[i], fsdp=p)

    def take_res(i):
        @pl.when(g * FG + i != f)
        def _():
            re_got(i).wait_recv()

    attn = attn_own[...]
    for e in (near, far, both):
        rs_got(e).wait_recv()
        attn = attn + rs_in[e].astype(F32)
    loop(0, FG, take_res)
    h_all[f, pl.ds(g * FG, FG)] = (res_in[...].astype(F32) + attn).astype(BF16)

    def chunk(p, e):
        return h_all.at[p, pl.ds(e * FG, FG)]

    def hz_copy(i):
        return copy(chunk(f, g), chunk(f, g), hz_s.at[i], hz_r.at[f], fsdp=peer(i))

    def hz_got(i):
        p = peer(i)
        return copy(chunk(p, g), chunk(p, g), hz_s.at[i], hz_r.at[p], fsdp=p)

    def hx_copy(k):
        p = peer(k)
        return copy(chunk(p, g), chunk(p, g), hx_s.at[k], hx_r.at[k], expert=far)

    def hx_got(k):
        p = peer(k)
        return copy(chunk(p, far), chunk(p, far), hx_s.at[k], hx_r.at[k], expert=far)

    def hc_copy(k, t):
        p = peer(k)
        c = chunk(p, (g, far)[t])
        return copy(c, c, hc_s.at[k, t], hc_r.at[k, t], expert=near)

    def hc_got(k, t):
        p = peer(k)
        c = chunk(p, (near, both)[t])
        return copy(c, c, hc_s.at[k, t], hc_r.at[k, t], expert=near)

    def forward(n):
        hz_got(n).wait_recv()
        hx_copy(n).start()
        hc_copy(n, 0).start()

    hx_copy(0).start()
    hz_copy(1).start()
    hc_copy(0, 0).start()
    inner = lax.rem(lax.div(lax.rem(f, 4) + 1, 2), 2) == 1
    pl.when(inner)(lambda: hz_copy(2).start())
    hz_copy(1).wait_send()
    pl.when(jnp.logical_not(inner))(lambda: hz_copy(2).start())
    forward(1)
    loop(3, F, lambda i: hz_copy(i).start())

    def step(k):
        p = peer(k)
        hx_got(k).wait_recv()
        hc_copy(k, 1).start()
        hc_got(k, 0).wait_recv()
        hc_got(k, 1).wait_recv()
        gain = gain_ref[p]

        def dispatch(s):
            rows = jnp.dot(oh[s, :, :Q].astype(BF16), h_all[p, s], preferred_element_type=F32)
            at = s * CAP if isinstance(s, int) else pl.multiple_of(s * CAP, 8)
            square = jnp.sum(rows * rows, axis=1, keepdims=True)
            rows = rows * gain
            for e in range(2):
                lhs[e, pl.ds(at, CAP), :] = rows[e * CAP:(e + 1) * CAP]
                ssq[e, pl.ds(at, CAP), :] += jnp.broadcast_to(square[e * CAP:(e + 1) * CAP], (CAP, 128))

        loop(0, F, dispatch)
        two = k % 2
        copies = w_copies(k)
        for e in range(2):
            x = lhs[e].astype(BF16)
            for t in range(2):
                copies[2 * e + t].wait()
                y = jnp.dot(x, wslot[two, 2 * e + t], preferred_element_type=F32)
                if isinstance(k, int) and k == 0:
                    acc[e, t] = y
                else:
                    acc[e, t] += y
            if e == 0:
                when(k + 2 < F, lambda: forward(k + 2))

        def refill():
            for c in w_copies(k + 2):
                c.start()

        when(k + 2 < F, refill)

    if F > 8:
        acc[...] = jnp.zeros_like(acc)
    loop(0, F, step)

    for e in range(2):
        scale = lax.rsqrt(ssq[e][:, :1] / D + EPS)
        gate = acc[e, 0] * scale
        up = acc[e, 1] * scale
        hid[e] = (gate / (1.0 + jnp.exp(-gate)) * up).astype(BF16)

    def a_copy(hh, t):
        return copy(cbuf.at[hh, 0], a_in.at[hh, t], a_s.at[hh, t], a_r.at[hh, t], expert=near)

    def b_copy(hh, s):
        return copy(cbuf.at[hh, 1, s], b_in.at[hh, s], b_s.at[hh, s], b_r.at[hh, s], expert=far)

    def c_copy(hh, s):
        return copy(cbuf.at[hh, 2, s], c_in.at[hh, f], c_s.at[hh, s], c_r.at[hh, f], fsdp=s)

    def c_got(hh, p):
        return copy(c_in.at[hh, p], c_in.at[hh, p], c_s.at[hh, p], c_r.at[hh, p], fsdp=p)

    def order(n):
        return peer(F - 1 - n)

    def down(n):
        hh, i = n // 4, n % 4
        copies = d_copies(n)
        for e in range(2):
            copies[e].wait()
            ybuf[e] = jnp.dot(hid[e], dslot[n % D_SLOTS, e], preferred_element_type=F32)
        if n + D_SLOTS < 4 * HALVES:
            for c in d_copies(n + D_SLOTS):
                c.start()
        if i in (1, 3):
            a_copy(hh, i // 2).wait_recv()
        if i == 2:
            a_copy(hh, 0).wait_send()

        def combine(m):
            s = order(m)
            at = pl.multiple_of(s * CAP, 8)
            ys = jnp.concatenate([ybuf[0, pl.ds(at, CAP), :], ybuf[1, pl.ds(at, CAP), :]], axis=0)
            ys = (ys * oh[s, :, Q:Q + 1]).astype(BF16)
            c = lax.dot_general(
                oh[s, :, :Q].astype(BF16), ys, (((0,), (0,)), ((), ())), preferred_element_type=F32)
            if i in (1, 3):
                c = c + a_in[hh, i // 2, s].astype(F32)
            cbuf[hh, (0, 1, 0, 2)[i], s] = c.astype(BF16)
            if i == 1:
                b_copy(hh, s).start()

        loop(0, F, combine)
        if i in (0, 2):
            a_copy(hh, i // 2).start()

    def send_seq(hh, m):
        s = order(m)
        b_copy(hh, s).wait_recv()
        cbuf[hh, 2, s] = (cbuf[hh, 2, s].astype(F32) + b_in[hh, s].astype(F32)).astype(BF16)
        c_copy(hh, s).start()

    for hh in range(HALVES):
        for i in range(4):
            down(4 * hh + i)
            if hh > 0 and i in (0, 1) and F > 2:
                send_seq(hh - 1, i)
        if hh > 0:
            loop(2 if F > 2 else 0, F - 1, lambda m: send_seq(hh - 1, m))
    loop(0, F - 1, lambda m: send_seq(HALVES - 1, m))

    for hh in range(HALVES):
        b_copy(hh, f).wait_recv()
        ybuf[0, 0:Q, :] = cbuf[hh, 2, f].astype(F32) + b_in[hh, f].astype(F32)

        def add_seq(i):
            p = peer(i)
            c_got(hh, p).wait_recv()
            ybuf[0, 0:Q, :] += c_in[hh, p].astype(F32)

        loop(1, F, add_seq)
        width = min(C, CH)
        for i in range(CH // width):
            at = hh * CH + i * width
            state = h_all[g * FG + at // C, f, :, at % C:at % C + width].astype(F32)
            out_ref[:, at:at + width] = (state + ybuf[0, 0:Q, i * width:(i + 1) * width]).astype(BF16)

    def drain(i):
        rt_copy(i).wait_send()
        hs_copy(i).wait_send()
        for hh in range(HALVES):
            c_copy(hh, peer(i)).wait_send()

    loop(1, F, drain)
    loop(2, F, lambda i: hz_copy(i).wait_send())

    @pl.when(own_part)
    def _():
        loop(1, F, lambda i: re_copy(i).wait_send())

    for e in (near, far, both):
        rs_copy(e).wait_send()

    def drain_all(k):
        hx_copy(k).wait_send()
        hc_copy(k, 0).wait_send()
        hc_copy(k, 1).wait_send()
        for hh in range(HALVES):
            b_copy(hh, k).wait_send()

    loop(0, F, drain_all)
    for hh in range(HALVES):
        a_copy(hh, 1).wait_send()


def layer(F, G, queries, keys, values, out_weight, residual, norm_gain,
          route_ids, route_slots, route_weights, w_gate, w_up, w_down):
    Q = queries.shape[0]
    D = residual.shape[1]
    C = out_weight.shape[1]
    H = w_gate.shape[2]
    R = CAP * F
    FG = F // G
    C2 = D // G
    CH = C2 // HALVES
    gain = norm_gain.reshape(F, 1, C)
    vm = pl.BlockSpec(memory_space=pltpu.VMEM)
    hbm = pl.BlockSpec(memory_space=pltpu.HBM)
    dma = pltpu.SemaphoreType.DMA
    return pl.pallas_call(
        functools.partial(kernel, F, G),
        out_shape=jax.ShapeDtypeStruct((Q, C2), BF16),
        in_specs=[hbm] * 5 + [vm] * 4 + [hbm] * 3,
        out_specs=vm,
        scratch_shapes=[
            pltpu.VMEM(queries.shape, BF16),
            pltpu.VMEM(keys.shape[1:], BF16),
            pltpu.VMEM(values.shape[1:], BF16),
            pltpu.VMEM(out_weight.shape, BF16),
            pltpu.VMEM(residual.shape, BF16),
            pltpu.VMEM((F, Q, queries.shape[1]), BF16),
            pltpu.VMEM((F, 8, 128), jnp.int32),
            pltpu.VMEM((FG, Q, C), BF16),
            pltpu.VMEM((G, FG, Q, C), BF16),
            pltpu.VMEM((G, FG, Q, C), BF16),
            pltpu.VMEM((FG, Q, C), F32),
            pltpu.VMEM((F, F, Q, C), BF16),
            pltpu.VMEM((F, 2 * CAP, 128), F32),
            pltpu.VMEM((2, R, C), F32),
            pltpu.VMEM((2, R, 128), F32),
            pltpu.VMEM((2, 2, R, H), F32),
            pltpu.VMEM((2, R, H), BF16),
            pltpu.VMEM((2, R, CH), F32),
            pltpu.VMEM((HALVES, 3, F, Q, CH), BF16),
            pltpu.VMEM((HALVES, 2, F, Q, CH), BF16),
            pltpu.VMEM((HALVES, F, Q, CH), BF16),
            pltpu.VMEM((HALVES, F, Q, CH), BF16),
            pltpu.VMEM((2, 4, C, H), BF16),
            pltpu.VMEM((D_SLOTS, 2, H, CH), BF16),
            dma((5,)), dma((F,)), dma((F,)), dma((F,)), dma((F,)), dma((F,)), dma((FG,)),
            dma((G,)), dma((G,)), dma((F,)), dma((F,)), dma((F,)), dma((F,)),
            dma((F, 2)), dma((F, 2)), dma((HALVES, 2)), dma((HALVES, 2)), dma((HALVES, F)), dma((HALVES, F)),
            dma((HALVES, F)), dma((HALVES, F)), dma((2, 4)), dma((D_SLOTS, 2)),
        ],
        compiler_params=pltpu.CompilerParams(
            collective_id=0, has_side_effects=True, vmem_limit_bytes=67043328),
    )(queries, keys[0], values[0], out_weight, residual, gain,
      route_ids.T, route_slots.T, route_weights.T, w_gate, w_up, w_down)


def solution(mesh):
    F, G = mesh.shape["fsdp"], mesh.shape["expert"]
    rows = P(("groups", "fsdp"), None)
    in_specs = (
        P(("groups", "fsdp"), "expert"),
        P(("groups", "fsdp"), None, "expert"),
        P(("groups", "fsdp"), None, "expert"),
        P("expert", "fsdp"),
        rows, P(), rows, rows, rows,
        P("expert", None, "fsdp"),
        P("expert", None, "fsdp"),
        P("expert", "fsdp", None),
    )
    return jax.shard_map(
        functools.partial(layer, F, G), mesh=mesh, in_specs=in_specs,
        out_specs=P(("groups", "fsdp"), "expert"), check_vma=False,
    )
```

```python
import functools

import jax
import jax.numpy as jnp
from jax import lax
from jax.experimental import pallas as pl
from jax.experimental.pallas import tpu as pltpu
from jax.sharding import PartitionSpec as P

HEAD_DIM = 128
CAP = 24
EPS = 1e-05
MESH = pl.DeviceIdType.MESH
F32 = jnp.float32
BF16 = jnp.bfloat16
HALVES = 2
D_SLOTS = 4
VMEM = 67043328


def loop(low, high, body):
    if high - low <= 8:
        for i in range(low, high):
            body(i)
    else:
        lax.fori_loop(low, high, lambda i, c: (body(i), c)[1], 0)


def when(cond, body):
    if isinstance(cond, bool):
        if cond:
            body()
    else:
        pl.when(cond)(body)


def kernel(
    F, G,
    q_hbm, k_hbm, v_hbm, ow_hbm, res_hbm, gain_ref, ids_ref, slots_ref, wts_ref, wg_ref, wu_ref, wd_ref,
    out_ref,
    q_ref, k_ref, v_ref, ow_ref, res_ref,
    heads, routes, res_in, part, rs_in, attn_own, h_all, oh, lhs, ssq, acc, hid, ybuf,
    abuf, cbuf, a_in, b_in, c_in, wslot, dslot,
    in_sem, hs_s, hs_r, rt_s, rt_r, re_s, re_r, rs_s, rs_r, hz_s, hz_r, hx_s, hx_r, hc_s, hc_r,
    a_s, a_r, b_s, b_r, c_s, c_r, w_sem, d_sem,
):
    f = lax.axis_index("fsdp")
    g = lax.axis_index("expert")
    FG = F // G
    Q = q_ref.shape[0]
    ctx = k_ref.shape[0]
    C = ow_ref.shape[1]
    D = wg_ref.shape[1]
    C2 = D // G
    CH = C2 // HALVES
    n_heads = q_ref.shape[1] // HEAD_DIM

    def flip(a, m, n):
        if isinstance(m, int) and m == 0:
            return a
        out = 0
        bit = 1
        while bit < n:
            low = lax.rem(lax.div(a, bit), 2)
            if isinstance(m, int):
                mine = (m // bit) % 2
                low = 1 - low if mine else low
            else:
                mine = lax.rem(lax.div(m, bit), 2)
                low = low + mine - 2 * low * mine
            out = out + bit * low
            bit *= 2
        return out

    def half(a):
        return a // 2 if isinstance(a, int) else lax.div(a, 2)

    def home(s):
        quarter = s // FG
        high = half(quarter)
        low = quarter - 2 * high
        return 2 * (low + high - 2 * low * high) + high

    def first_seq(e):
        high = half(e)
        low = e - 2 * high
        return (2 * low + high + low - 2 * high * low) * FG

    def slot(s):
        return home(s) * FG + s % FG

    def peer(i):
        if F & (F - 1) == 0:
            return flip(f, i, F)
        return lax.rem(f + i, F)

    def copy(src, dst, s, r, **dev):
        return pltpu.make_async_remote_copy(
            src_ref=src, dst_ref=dst, send_sem=s, recv_sem=r,
            device_id=dev, device_id_type=MESH,
        )

    barrier = pltpu.get_barrier_semaphore()

    def greet_f(i):
        pl.semaphore_signal(barrier, inc=1, device_id={"fsdp": lax.rem(f + i, F)}, device_id_type=MESH)

    loop(1, F, greet_f)
    for i in range(1, G):
        pl.semaphore_signal(
            barrier, inc=1, device_id={"expert": lax.rem(g + i, G)}, device_id_type=MESH)

    loads = [
        pltpu.make_async_copy(src, dst, in_sem.at[i])
        for i, (src, dst) in enumerate((
            (q_hbm, q_ref), (k_hbm, k_ref), (v_hbm, v_ref), (res_hbm, res_ref), (ow_hbm, ow_ref)))
    ]
    for c in loads:
        c.start()

    def w_copies(k):
        col = peer(k)
        rows = pl.ds(pl.multiple_of(col * C, C), C)
        two = k % 2
        out = []
        for e in range(2):
            for t, ref in enumerate((wg_ref, wu_ref)):
                out.append(pltpu.make_async_copy(
                    ref.at[e, rows, :], wslot.at[two, 2 * e + t], w_sem.at[two, 2 * e + t]))
        return out

    masks = (3, 1, 2, 0)

    def d_copies(n):
        block = flip(g, masks[n % 4], G)
        cols = pl.ds(pl.multiple_of(block * C2 + (n // 4) * CH, CH), CH)
        return [
            pltpu.make_async_copy(wd_ref.at[e, :, cols], dslot.at[n % D_SLOTS, e], d_sem.at[n % D_SLOTS, e])
            for e in range(2)
        ]

    routes[f] = jnp.zeros((8, 128), jnp.int32)
    for t, ref in enumerate((ids_ref, slots_ref, wts_ref)):
        routes[f, 2 * t:2 * t + 2, :Q] = ref[...]

    n_kv = k_ref.shape[1] // HEAD_DIM
    per = n_heads // n_kv
    rate = HEAD_DIM ** (-0.5) * 1.4426950408889634
    for c in loads:
        c.wait()
    for k in range(min(2, F)):
        for c in w_copies(k):
            c.start()
    for n in range(D_SLOTS):
        for c in d_copies(n):
            c.start()

    for kv in range(n_kv):
        cols = slice(kv * HEAD_DIM, (kv + 1) * HEAD_DIM)
        qs = jnp.concatenate(
            [q_ref[:, h * HEAD_DIM:(h + 1) * HEAD_DIM] for h in range(kv * per, (kv + 1) * per)], axis=0)
        s = lax.dot_general(qs, k_ref[:, cols], (((1,), (1,)), ((), ())), preferred_element_type=F32)
        tail = 128
        key_pos = ctx - tail + lax.broadcasted_iota(jnp.int32, (per, Q, tail), 2)
        query_pos = ctx - Q + lax.broadcasted_iota(jnp.int32, (per, Q, tail), 1)
        allowed = (key_pos <= query_pos).reshape(per * Q, tail)
        s = jnp.concatenate([s[:, :ctx - tail], jnp.where(allowed, s[:, ctx - tail:], -1e30)], axis=1)
        top = jnp.max(s, axis=1, keepdims=True)
        w = jnp.exp2((s - top) * rate)
        total = jnp.sum(w, axis=1, keepdims=True)
        o = jnp.dot(w.astype(BF16), v_ref[:, cols], preferred_element_type=F32) / total
        for n in range(per):
            h = kv * per + n
            heads[f, :, h * HEAD_DIM:(h + 1) * HEAD_DIM] = o[n * Q:(n + 1) * Q].astype(BF16)

    pl.semaphore_wait(barrier, F - 1 + G - 1)

    def rt_copy(i):
        return copy(routes.at[f], routes.at[f], rt_s.at[i], rt_r.at[f], fsdp=peer(i))

    def rt_got(i):
        p = peer(i)
        return copy(routes.at[p], routes.at[p], rt_s.at[i], rt_r.at[p], fsdp=p)

    def cols_of(p):
        return pl.ds(pl.multiple_of(p * C, C), C)

    own_part = home(f) == g
    mine = f % FG

    def re_copy(i):
        p = peer(i)
        return copy(res_ref.at[:, cols_of(p)], res_in.at[mine], re_s.at[i], re_r.at[mine], fsdp=p)

    def hs_copy(i):
        return copy(heads.at[f], heads.at[f], hs_s.at[i], hs_r.at[f], fsdp=peer(i))

    def hs_got(p):
        return copy(heads.at[p], heads.at[p], hs_s.at[0], hs_r.at[p], fsdp=p)

    loop(1, F, lambda i: hs_copy(i).start())
    loop(1, F, lambda i: rt_copy(i).start())

    def send_res():
        loop(1, F, lambda i: re_copy(F - i).start())
        res_in[mine] = res_ref[:, cols_of(f)]

    ssq[...] = jnp.zeros_like(ssq)

    def rs_copy(j):
        return copy(part.at[j], rs_in.at[g], rs_s.at[j], rs_r.at[g], expert=j)

    def rs_got(e):
        return copy(part.at[e], rs_in.at[e], rs_s.at[e], rs_r.at[e], expert=e)

    def project(i):
        base = flip(f // FG, i, G) * FG
        j = home(base)

        def arrive(n):
            p = base + n

            @pl.when(p != f)
            def _():
                hs_got(p).wait_recv()

        loop(0, FG, arrive)
        rows = heads[pl.ds(base, FG)].reshape(FG * Q, n_heads * HEAD_DIM)
        y = jnp.dot(rows, ow_ref[...], preferred_element_type=F32).reshape(FG, Q, C)

        @pl.when(j == g)
        def _():
            attn_own[...] = y

        @pl.when(j != g)
        def _():
            part[j] = y.astype(BF16)
            rs_copy(j).start()

    for i in range(G):
        project(i)
        if i == 1:
            pl.when(own_part)(send_res)

    loop(1, F, lambda i: rt_got(i).wait_recv())

    def tables(s):
        r = routes[s]
        slot_row = lax.broadcasted_iota(jnp.int32, (2 * CAP, Q), 0)
        table = jnp.zeros((2 * CAP, Q), F32)
        weight = jnp.zeros((2 * CAP, Q), F32)
        for t in range(2):
            within = r[t:t + 1, :Q] - 2 * g
            inside = (within >= 0) & (within < 2)
            row = jnp.where(inside, r[2 + t:3 + t, :Q] + CAP * within, -1)
            hit = (row == slot_row).astype(F32)
            table = table + hit
            weight = weight + hit * (r[4 + t:5 + t, :Q].astype(F32) / 65536.0)
        oh[s, :, :Q] = table
        oh[s, :, Q:] = jnp.broadcast_to(jnp.sum(weight, axis=1, keepdims=True), (2 * CAP, 128 - Q))

    loop(0, F, tables)

    far, near, both = flip(g, 2, G), flip(g, 1, G), flip(g, 3, G)

    def re_got(i):
        p = first_seq(g) + i
        return copy(res_in.at[i], res_in.at[i], re_s.at[0], re_r.at[i], fsdp=p)

    def take_res(i):
        @pl.when(first_seq(g) + i != f)
        def _():
            re_got(i).wait_recv()

    attn = attn_own[...]
    for e in (near, far, both):
        rs_got(e).wait_recv()
        attn = attn + rs_in[e].astype(F32)
    loop(0, FG, take_res)
    h_all[f, pl.ds(g * FG, FG)] = (res_in[...].astype(F32) + attn).astype(BF16)

    def chunk(p, e):
        return h_all.at[p, pl.ds(e * FG, FG)]

    def hz_copy(i):
        return copy(chunk(f, g), chunk(f, g), hz_s.at[i], hz_r.at[f], fsdp=peer(i))

    def hz_got(i):
        p = peer(i)
        return copy(chunk(p, g), chunk(p, g), hz_s.at[i], hz_r.at[p], fsdp=p)

    def hx_copy(k):
        p = peer(k)
        return copy(chunk(p, g), chunk(p, g), hx_s.at[k], hx_r.at[k], expert=far)

    def hx_got(k):
        p = peer(k)
        return copy(chunk(p, far), chunk(p, far), hx_s.at[k], hx_r.at[k], expert=far)

    def hc_copy(k, t):
        p = peer(k)
        c = chunk(p, (g, far)[t])
        return copy(c, c, hc_s.at[k, t], hc_r.at[k, t], expert=near)

    def hc_got(k, t):
        p = peer(k)
        c = chunk(p, (near, both)[t])
        return copy(c, c, hc_s.at[k, t], hc_r.at[k, t], expert=near)

    def forward(n):
        hz_got(n).wait_recv()
        hx_copy(n).start()
        hc_copy(n, 0).start()

    hx_copy(0).start()
    hz_copy(1).start()
    hc_copy(0, 0).start()
    inner = lax.rem(lax.div(lax.rem(f, 4) + 1, 2), 2) == 1
    pl.when(inner)(lambda: hz_copy(2).start())
    hz_copy(1).wait_send()
    pl.when(jnp.logical_not(inner))(lambda: hz_copy(2).start())
    forward(1)
    loop(3, F, lambda i: hz_copy(i).start())

    def step(k):
        p = peer(k)
        hx_got(k).wait_recv()
        hc_copy(k, 1).start()
        hc_got(k, 0).wait_recv()
        hc_got(k, 1).wait_recv()
        gain = gain_ref[p]

        def dispatch(s):
            rows = jnp.dot(oh[s, :, :Q].astype(BF16), h_all[p, slot(s)], preferred_element_type=F32)
            at = s * CAP if isinstance(s, int) else pl.multiple_of(s * CAP, 8)
            square = jnp.sum(rows * rows, axis=1, keepdims=True)
            rows = rows * gain
            for e in range(2):
                lhs[e, pl.ds(at, CAP), :] = rows[e * CAP:(e + 1) * CAP]
                ssq[e, pl.ds(at, CAP), :] += jnp.broadcast_to(square[e * CAP:(e + 1) * CAP], (CAP, 128))

        loop(0, F, dispatch)
        two = k % 2
        for c in w_copies(k):
            c.wait()
        for e in range(2):
            x = lhs[e].astype(BF16)
            for t in range(2):
                y = jnp.dot(x, wslot[two, 2 * e + t], preferred_element_type=F32)
                if isinstance(k, int) and k == 0:
                    acc[e, t] = y
                else:
                    acc[e, t] += y
            if e == 0:
                when(k + 2 < F, lambda: forward(k + 2))

        def refill():
            for c in w_copies(k + 2):
                c.start()

        when(k + 2 < F, refill)

    if F > 8:
        acc[...] = jnp.zeros_like(acc)
    loop(0, F, step)

    for e in range(2):
        scale = lax.rsqrt(ssq[e][:, :1] / D + EPS)
        gate = acc[e, 0] * scale
        up = acc[e, 1] * scale
        hid[e] = (gate / (1.0 + jnp.exp(-gate)) * up).astype(BF16)

    def a_copy(hh, t):
        return copy(abuf.at[t], a_in.at[hh, t], a_s.at[hh, t], a_r.at[hh, t], expert=near)

    def b_copy(hh, s):
        return copy(cbuf.at[hh, 0, s], b_in.at[hh, s], b_s.at[hh, s], b_r.at[hh, s], expert=far)

    def c_copy(hh, s):
        return copy(cbuf.at[hh, 1, s], c_in.at[hh, f], c_s.at[hh, s], c_r.at[hh, f], fsdp=s)

    def c_got(hh, p):
        return copy(c_in.at[hh, p], c_in.at[hh, p], c_s.at[hh, p], c_r.at[hh, p], fsdp=p)

    def order(n):
        return peer(F - 1 - n)

    def down(n):
        hh, i = n // 4, n % 4
        for c in d_copies(n):
            c.wait()
        for e in range(2):
            ybuf[e] = jnp.dot(hid[e], dslot[n % D_SLOTS, e], preferred_element_type=F32)
        if n + D_SLOTS < 4 * HALVES:
            for c in d_copies(n + D_SLOTS):
                c.start()
        if i in (2, 3):
            a_copy(hh, i - 2).wait_recv()

        def combine(m):
            s = order(m)
            at = pl.multiple_of(s * CAP, 8)
            ys = jnp.concatenate([ybuf[0, pl.ds(at, CAP), :], ybuf[1, pl.ds(at, CAP), :]], axis=0)
            ys = (ys * oh[s, :, Q:Q + 1]).astype(BF16)
            c = lax.dot_general(
                oh[s, :, :Q].astype(BF16), ys, (((0,), (0,)), ((), ())), preferred_element_type=F32)
            if i in (2, 3):
                c = c + a_in[hh, i - 2, s].astype(F32)
            if i < 2:
                abuf[i, s] = c.astype(BF16)
            else:
                cbuf[hh, i - 2, s] = c.astype(BF16)

        if i < 2 and hh > 0:
            a_copy(hh - 1, i).wait_send()
        loop(0, F, combine)
        if i < 2:
            a_copy(hh, i).start()
        if i == 2:
            loop(0, F, lambda m: b_copy(hh, order(m)).start())

    def send_seq(hh, m):
        s = order(m)
        b_copy(hh, s).wait_recv()
        cbuf[hh, 1, s] = (cbuf[hh, 1, s].astype(F32) + b_in[hh, s].astype(F32)).astype(BF16)
        c_copy(hh, s).start()

    for hh in range(HALVES):
        for i in range(4):
            down(4 * hh + i)
            if hh > 0:
                loop((F - 1) * i // 4, (F - 1) * (i + 1) // 4, lambda m: send_seq(hh - 1, m))
    loop(0, F - 1, lambda m: send_seq(HALVES - 1, m))

    for hh in range(HALVES):
        b_copy(hh, f).wait_recv()
        ybuf[0, 0:Q, :] = cbuf[hh, 1, f].astype(F32) + b_in[hh, f].astype(F32)

        def add_seq(i):
            p = peer(i)
            c_got(hh, p).wait_recv()
            ybuf[0, 0:Q, :] += c_in[hh, p].astype(F32)

        loop(1, F, add_seq)
        width = min(C, CH)
        for i in range(CH // width):
            at = hh * CH + i * width
            state = h_all[g * FG + at // C, slot(f), :, at % C:at % C + width].astype(F32)
            out_ref[:, at:at + width] = (state + ybuf[0, 0:Q, i * width:(i + 1) * width]).astype(BF16)

    def drain(i):
        rt_copy(i).wait_send()
        hs_copy(i).wait_send()
        for hh in range(HALVES):
            c_copy(hh, peer(i)).wait_send()

    loop(1, F, drain)
    loop(2, F, lambda i: hz_copy(i).wait_send())

    @pl.when(own_part)
    def _():
        loop(1, F, lambda i: re_copy(i).wait_send())

    for e in (near, far, both):
        rs_copy(e).wait_send()

    def drain_all(k):
        hx_copy(k).wait_send()
        hc_copy(k, 0).wait_send()
        hc_copy(k, 1).wait_send()
        for hh in range(HALVES):
            b_copy(hh, k).wait_send()

    loop(0, F, drain_all)
    for t in range(2):
        a_copy(HALVES - 1, t).wait_send()


def layer(F, G, queries, keys, values, out_weight, residual, norm_gain,
          route_ids, route_slots, route_weights, w_gate, w_up, w_down):
    Q = queries.shape[0]
    D = residual.shape[1]
    C = out_weight.shape[1]
    H = w_gate.shape[2]
    R = CAP * F
    FG = F // G
    C2 = D // G
    CH = C2 // HALVES
    gain = norm_gain.reshape(F, 1, C)
    vm = pl.BlockSpec(memory_space=pltpu.VMEM)
    hbm = pl.BlockSpec(memory_space=pltpu.HBM)
    dma = pltpu.SemaphoreType.DMA
    return pl.pallas_call(
        functools.partial(kernel, F, G),
        out_shape=jax.ShapeDtypeStruct((Q, C2), BF16),
        in_specs=[hbm] * 5 + [vm] * 4 + [hbm] * 3,
        out_specs=vm,
        scratch_shapes=[
            pltpu.VMEM(queries.shape, BF16),
            pltpu.VMEM(keys.shape[1:], BF16),
            pltpu.VMEM(values.shape[1:], BF16),
            pltpu.VMEM(out_weight.shape, BF16),
            pltpu.VMEM(residual.shape, BF16),
            pltpu.VMEM((F, Q, queries.shape[1]), BF16),
            pltpu.VMEM((F, 8, 128), jnp.int32),
            pltpu.VMEM((FG, Q, C), BF16),
            pltpu.VMEM((G, FG, Q, C), BF16),
            pltpu.VMEM((G, FG, Q, C), BF16),
            pltpu.VMEM((FG, Q, C), F32),
            pltpu.VMEM((F, F, Q, C), BF16),
            pltpu.VMEM((F, 2 * CAP, 128), F32),
            pltpu.VMEM((2, R, C), F32),
            pltpu.VMEM((2, R, 128), F32),
            pltpu.VMEM((2, 2, R, H), F32),
            pltpu.VMEM((2, R, H), BF16),
            pltpu.VMEM((2, R, CH), F32),
            pltpu.VMEM((2, F, Q, CH), BF16),
            pltpu.VMEM((HALVES, 2, F, Q, CH), BF16),
            pltpu.VMEM((HALVES, 2, F, Q, CH), BF16),
            pltpu.VMEM((HALVES, F, Q, CH), BF16),
            pltpu.VMEM((HALVES, F, Q, CH), BF16),
            pltpu.VMEM((2, 4, C, H), BF16),
            pltpu.VMEM((D_SLOTS, 2, H, CH), BF16),
            dma((5,)), dma((F,)), dma((F,)), dma((F,)), dma((F,)), dma((F,)), dma((FG,)),
            dma((G,)), dma((G,)), dma((F,)), dma((F,)), dma((F,)), dma((F,)),
            dma((F, 2)), dma((F, 2)), dma((HALVES, 2)), dma((HALVES, 2)), dma((HALVES, F)), dma((HALVES, F)),
            dma((HALVES, F)), dma((HALVES, F)), dma((2, 4)), dma((D_SLOTS, 2)),
        ],
        compiler_params=pltpu.CompilerParams(
            collective_id=0, has_side_effects=True, vmem_limit_bytes=VMEM),
    )(queries, keys[0], values[0], out_weight, residual, gain,
      route_ids.T, route_slots.T, route_weights.T, w_gate, w_up, w_down)


def solution(mesh):
    F, G = mesh.shape["fsdp"], mesh.shape["expert"]
    rows = P(("groups", "fsdp"), None)
    in_specs = (
        P(("groups", "fsdp"), "expert"),
        P(("groups", "fsdp"), None, "expert"),
        P(("groups", "fsdp"), None, "expert"),
        P("expert", "fsdp"),
        rows, P(), rows, rows, rows,
        P("expert", None, "fsdp"),
        P("expert", None, "fsdp"),
        P("expert", "fsdp", None),
    )
    return jax.shard_map(
        functools.partial(layer, F, G), mesh=mesh, in_specs=in_specs,
        out_specs=P(("groups", "fsdp"), "expert"), check_vma=False,
    )
```

```python
import functools

import jax
import jax.numpy as jnp
from jax import lax
from jax.experimental import pallas as pl
from jax.experimental.pallas import tpu as pltpu
from jax.sharding import PartitionSpec as P

HEAD_DIM = 128
CAP = 24
EPS = 1e-05
MESH = pl.DeviceIdType.MESH
F32 = jnp.float32
BF16 = jnp.bfloat16
HALVES = 2
D_SLOTS = 4
VMEM = 67043328


def loop(low, high, body):
    if high - low <= 8:
        for i in range(low, high):
            body(i)
    else:
        lax.fori_loop(low, high, lambda i, c: (body(i), c)[1], 0)


def when(cond, body):
    if isinstance(cond, bool):
        if cond:
            body()
    else:
        pl.when(cond)(body)


def kernel(
    F, G,
    q_hbm, k_hbm, v_hbm, ow_hbm, res_hbm, gain_ref, ids_ref, slots_ref, wts_ref, wg_ref, wu_ref, wd_ref,
    out_ref,
    q_ref, k_ref, v_ref, ow_ref, res_ref,
    heads, routes, res_in, part, rs_in, attn_own, h_all, oh, lhs, ssq, acc, hid, ybuf,
    abuf, cbuf, a_in, b_in, c_in, wslot, dslot,
    in_sem, hs_s, hs_r, rt_s, rt_r, re_s, re_r, rs_s, rs_r, hz_s, hz_r, hx_s, hx_r, hc_s, hc_r,
    a_s, a_r, b_s, b_r, c_s, c_r, w_sem, d_sem,
):
    f = lax.axis_index("fsdp")
    g = lax.axis_index("expert")
    FG = F // G
    Q = q_ref.shape[0]
    ctx = k_ref.shape[0]
    C = ow_ref.shape[1]
    D = wg_ref.shape[1]
    C2 = D // G
    CH = C2 // HALVES
    n_heads = q_ref.shape[1] // HEAD_DIM

    def flip(a, m, n):
        if isinstance(m, int) and m == 0:
            return a
        out = 0
        bit = 1
        while bit < n:
            low = lax.rem(lax.div(a, bit), 2)
            if isinstance(m, int):
                mine = (m // bit) % 2
                low = 1 - low if mine else low
            else:
                mine = lax.rem(lax.div(m, bit), 2)
                low = low + mine - 2 * low * mine
            out = out + bit * low
            bit *= 2
        return out

    def half(a):
        return a // 2 if isinstance(a, int) else lax.div(a, 2)

    def home(s):
        quarter = s // FG
        high = half(quarter)
        low = quarter - 2 * high
        return 2 * (low + high - 2 * low * high) + high

    def first_seq(e):
        high = half(e)
        low = e - 2 * high
        return (2 * low + high + low - 2 * high * low) * FG

    def slot(s):
        return home(s) * FG + s % FG

    def peer(i):
        if F & (F - 1) == 0:
            return flip(f, i, F)
        return lax.rem(f + i, F)

    def copy(src, dst, s, r, **dev):
        return pltpu.make_async_remote_copy(
            src_ref=src, dst_ref=dst, send_sem=s, recv_sem=r,
            device_id=dev, device_id_type=MESH,
        )

    barrier = pltpu.get_barrier_semaphore()

    def greet_f(i):
        pl.semaphore_signal(barrier, inc=1, device_id={"fsdp": lax.rem(f + i, F)}, device_id_type=MESH)

    loop(1, F, greet_f)
    for i in range(1, G):
        pl.semaphore_signal(
            barrier, inc=1, device_id={"expert": lax.rem(g + i, G)}, device_id_type=MESH)

    loads = [
        pltpu.make_async_copy(src, dst, in_sem.at[i])
        for i, (src, dst) in enumerate((
            (q_hbm, q_ref), (k_hbm, k_ref), (v_hbm, v_ref), (res_hbm, res_ref), (ow_hbm, ow_ref)))
    ]
    for c in loads:
        c.start()

    def w_copies(k):
        col = peer(k)
        rows = pl.ds(pl.multiple_of(col * C, C), C)
        two = k % 2
        out = []
        for e in range(2):
            for t, ref in enumerate((wg_ref, wu_ref)):
                out.append(pltpu.make_async_copy(
                    ref.at[e, rows, :], wslot.at[two, 2 * e + t], w_sem.at[two, 2 * e + t]))
        return out

    masks = (3, 1, 2, 0)

    def d_copies(n):
        block = flip(g, masks[n % 4], G)
        cols = pl.ds(pl.multiple_of(block * C2 + (n // 4) * CH, CH), CH)
        return [
            pltpu.make_async_copy(wd_ref.at[e, :, cols], dslot.at[n % D_SLOTS, e], d_sem.at[n % D_SLOTS, e])
            for e in range(2)
        ]

    routes[f] = jnp.zeros((8, 128), jnp.int32)
    for t, ref in enumerate((ids_ref, slots_ref, wts_ref)):
        routes[f, 2 * t:2 * t + 2, :Q] = ref[...]

    n_kv = k_ref.shape[1] // HEAD_DIM
    per = n_heads // n_kv
    rate = HEAD_DIM ** (-0.5) * 1.4426950408889634
    for c in loads:
        c.wait()
    for k in range(min(2, F)):
        for c in w_copies(k):
            c.start()
    for n in range(D_SLOTS):
        for c in d_copies(n):
            c.start()

    for kv in range(n_kv):
        cols = slice(kv * HEAD_DIM, (kv + 1) * HEAD_DIM)
        qs = jnp.concatenate(
            [q_ref[:, h * HEAD_DIM:(h + 1) * HEAD_DIM] for h in range(kv * per, (kv + 1) * per)], axis=0)
        s = lax.dot_general(qs, k_ref[:, cols], (((1,), (1,)), ((), ())), preferred_element_type=F32)
        tail = 128
        key_pos = ctx - tail + lax.broadcasted_iota(jnp.int32, (per, Q, tail), 2)
        query_pos = ctx - Q + lax.broadcasted_iota(jnp.int32, (per, Q, tail), 1)
        allowed = (key_pos <= query_pos).reshape(per * Q, tail)
        s = jnp.concatenate([s[:, :ctx - tail], jnp.where(allowed, s[:, ctx - tail:], -1e30)], axis=1)
        top = jnp.max(s, axis=1, keepdims=True)
        w = jnp.exp2((s - top) * rate)
        total = jnp.sum(w, axis=1, keepdims=True)
        o = jnp.dot(w.astype(BF16), v_ref[:, cols], preferred_element_type=F32) / total
        for n in range(per):
            h = kv * per + n
            heads[f, :, h * HEAD_DIM:(h + 1) * HEAD_DIM] = o[n * Q:(n + 1) * Q].astype(BF16)

    pl.semaphore_wait(barrier, F - 1 + G - 1)

    def rt_copy(i):
        return copy(routes.at[f], routes.at[f], rt_s.at[i], rt_r.at[f], fsdp=peer(i))

    def rt_got(i):
        p = peer(i)
        return copy(routes.at[p], routes.at[p], rt_s.at[i], rt_r.at[p], fsdp=p)

    def cols_of(p):
        return pl.ds(pl.multiple_of(p * C, C), C)

    own_part = home(f) == g
    mine = f % FG

    def re_copy(i):
        p = peer(i)
        return copy(res_ref.at[:, cols_of(p)], res_in.at[mine], re_s.at[i], re_r.at[mine], fsdp=p)

    def hs_copy(i):
        return copy(heads.at[f], heads.at[f], hs_s.at[i], hs_r.at[f], fsdp=peer(i))

    def hs_got(p):
        return copy(heads.at[p], heads.at[p], hs_s.at[0], hs_r.at[p], fsdp=p)

    loop(1, F, lambda i: hs_copy(i).start())
    loop(1, F, lambda i: rt_copy(i).start())

    def send_res():
        loop(1, F, lambda i: re_copy(i).start())
        res_in[mine] = res_ref[:, cols_of(f)]

    ssq[...] = jnp.zeros_like(ssq)

    def rs_copy(j):
        return copy(part.at[j], rs_in.at[g], rs_s.at[j], rs_r.at[g], expert=j)

    def rs_got(e):
        return copy(part.at[e], rs_in.at[e], rs_s.at[e], rs_r.at[e], expert=e)

    def project(i):
        base = flip(f // FG, i, G) * FG
        j = home(base)

        def arrive(n):
            p = base + n

            @pl.when(p != f)
            def _():
                hs_got(p).wait_recv()

        loop(0, FG, arrive)
        rows = heads[pl.ds(base, FG)].reshape(FG * Q, n_heads * HEAD_DIM)
        y = jnp.dot(rows, ow_ref[...], preferred_element_type=F32).reshape(FG, Q, C)

        @pl.when(j == g)
        def _():
            attn_own[...] = y

        @pl.when(j != g)
        def _():
            part[j] = y.astype(BF16)
            rs_copy(j).start()

    for i in range(G):
        project(i)
        if i == 1:
            pl.when(own_part)(send_res)

    loop(1, F, lambda i: rt_got(i).wait_recv())

    def tables(s):
        r = routes[s]
        slot_row = lax.broadcasted_iota(jnp.int32, (2 * CAP, Q), 0)
        table = jnp.zeros((2 * CAP, Q), F32)
        weight = jnp.zeros((2 * CAP, Q), F32)
        for t in range(2):
            within = r[t:t + 1, :Q] - 2 * g
            inside = (within >= 0) & (within < 2)
            row = jnp.where(inside, r[2 + t:3 + t, :Q] + CAP * within, -1)
            hit = (row == slot_row).astype(F32)
            table = table + hit
            weight = weight + hit * (r[4 + t:5 + t, :Q].astype(F32) / 65536.0)
        oh[s, :, :Q] = table
        oh[s, :, Q:] = jnp.broadcast_to(jnp.sum(weight, axis=1, keepdims=True), (2 * CAP, 128 - Q))

    loop(0, F, tables)

    far, near, both = flip(g, 2, G), flip(g, 1, G), flip(g, 3, G)

    def re_got(i):
        p = first_seq(g) + i
        return copy(res_in.at[i], res_in.at[i], re_s.at[0], re_r.at[i], fsdp=p)

    def take_res(i):
        @pl.when(first_seq(g) + i != f)
        def _():
            re_got(i).wait_recv()

    attn = attn_own[...]
    for e in (near, far, both):
        rs_got(e).wait_recv()
        attn = attn + rs_in[e].astype(F32)
    loop(0, FG, take_res)
    h_all[f, pl.ds(g * FG, FG)] = (res_in[...].astype(F32) + attn).astype(BF16)

    def chunk(p, e):
        return h_all.at[p, pl.ds(e * FG, FG)]

    pieces = 2 if C % 256 == 0 else 1
    CP = C // pieces

    def piece(p, e, t):
        return h_all.at[p, pl.ds(e * FG, FG), :, pl.ds(t * CP, CP)]

    def hz_copy(i, t):
        return copy(piece(f, g, t), piece(f, g, t), hz_s.at[i, t], hz_r.at[f, t], fsdp=peer(i))

    def hz_got(i, t):
        p = peer(i)
        return copy(piece(p, g, t), piece(p, g, t), hz_s.at[i, t], hz_r.at[p, t], fsdp=p)

    def hx_copy(k, t):
        p = peer(k)
        return copy(piece(p, g, t), piece(p, g, t), hx_s.at[k, t], hx_r.at[k, t], expert=far)

    def hx_got(k, t):
        p = peer(k)
        return copy(piece(p, far, t), piece(p, far, t), hx_s.at[k, t], hx_r.at[k, t], expert=far)

    def hc_copy(k, t):
        p = peer(k)
        c = chunk(p, (g, far)[t])
        return copy(c, c, hc_s.at[k, t], hc_r.at[k, t], expert=near)

    def hc_got(k, t):
        p = peer(k)
        c = chunk(p, (near, both)[t])
        return copy(c, c, hc_s.at[k, t], hc_r.at[k, t], expert=near)

    def forward(n):
        for t in range(pieces):
            hz_got(n, t).wait_recv()
            hx_copy(n, t).start()
        hc_copy(n, 0).start()

    def spread(i):
        for t in range(pieces):
            hz_copy(i, t).start()

    for t in range(pieces):
        hx_copy(0, t).start()
    spread(1)
    hc_copy(0, 0).start()
    loop(2, F, spread)
    forward(1)

    def act(e):
        scale = lax.rsqrt(ssq[e][:, :1] / D + EPS)
        gate = acc[e, 0] * scale
        up = acc[e, 1] * scale
        hid[e] = (gate / (1.0 + jnp.exp(-gate)) * up).astype(BF16)

    def step(k):
        p = peer(k)
        for t in range(pieces):
            hx_got(k, t).wait_recv()
        hc_copy(k, 1).start()
        hc_got(k, 0).wait_recv()
        hc_got(k, 1).wait_recv()
        gain = gain_ref[p]

        def dispatch(s):
            rows = jnp.dot(oh[s, :, :Q].astype(BF16), h_all[p, slot(s)], preferred_element_type=F32)
            at = s * CAP if isinstance(s, int) else pl.multiple_of(s * CAP, 8)
            square = jnp.sum(rows * rows, axis=1, keepdims=True)
            rows = rows * gain
            for e in range(2):
                lhs[e, pl.ds(at, CAP), :] = rows[e * CAP:(e + 1) * CAP]
                ssq[e, pl.ds(at, CAP), :] += jnp.broadcast_to(square[e * CAP:(e + 1) * CAP], (CAP, 128))

        loop(0, F, dispatch)
        two = k % 2
        for c in w_copies(k):
            c.wait()
        for e in range(2):
            x = lhs[e].astype(BF16)
            for t in range(2):
                y = jnp.dot(x, wslot[two, 2 * e + t], preferred_element_type=F32)
                if isinstance(k, int) and k == 0:
                    acc[e, t] = y
                else:
                    acc[e, t] += y
            if isinstance(k, int) and k == F - 1:
                act(e)
            if e == 0:
                when(k + 2 < F, lambda: forward(k + 2))

        def refill():
            for c in w_copies(k + 2):
                c.start()

        when(k + 2 < F, refill)

    if F > 8:
        acc[...] = jnp.zeros_like(acc)
    for c in d_copies(0):
        c.wait()
    loop(0, F, step)

    if F > 8:
        for e in range(2):
            act(e)

    def a_copy(hh, t):
        return copy(abuf.at[t], a_in.at[hh, t], a_s.at[hh, t], a_r.at[hh, t], expert=near)

    def b_copy(hh, s):
        return copy(cbuf.at[hh, 0, s], b_in.at[hh, s], b_s.at[hh, s], b_r.at[hh, s], expert=far)

    def c_copy(hh, s):
        return copy(cbuf.at[hh, 1, s], c_in.at[hh, f], c_s.at[hh, s], c_r.at[hh, f], fsdp=s)

    def c_got(hh, p):
        return copy(c_in.at[hh, p], c_in.at[hh, p], c_s.at[hh, p], c_r.at[hh, p], fsdp=p)

    def order(n):
        return peer(F - 1 - n)

    def down(n):
        hh, i = n // 4, n % 4
        if n > 0:
            for c in d_copies(n):
                c.wait()
        for e in range(2):
            ybuf[e] = jnp.dot(hid[e], dslot[n % D_SLOTS, e], preferred_element_type=F32)
        if n + D_SLOTS < 4 * HALVES:
            for c in d_copies(n + D_SLOTS):
                c.start()
        if i in (2, 3):
            a_copy(hh, i - 2).wait_recv()

        def combine(m):
            s = order(m)
            at = pl.multiple_of(s * CAP, 8)
            ys = jnp.concatenate([ybuf[0, pl.ds(at, CAP), :], ybuf[1, pl.ds(at, CAP), :]], axis=0)
            ys = (ys * oh[s, :, Q:Q + 1]).astype(BF16)
            c = lax.dot_general(
                oh[s, :, :Q].astype(BF16), ys, (((0,), (0,)), ((), ())), preferred_element_type=F32)
            if i in (2, 3):
                c = c + a_in[hh, i - 2, s].astype(F32)
            if i < 2:
                abuf[i, s] = c.astype(BF16)
            else:
                cbuf[hh, i - 2, s] = c.astype(BF16)

        if i < 2 and hh > 0:
            a_copy(hh - 1, i).wait_send()
        loop(0, F, combine)
        if i < 2:
            a_copy(hh, i).start()
        if i == 2:
            loop(0, F, lambda m: b_copy(hh, order(m)).start())

    def send_seq(hh, m):
        s = order(m)
        b_copy(hh, s).wait_recv()
        cbuf[hh, 1, s] = (cbuf[hh, 1, s].astype(F32) + b_in[hh, s].astype(F32)).astype(BF16)
        c_copy(hh, s).start()

    for hh in range(HALVES):
        for i in range(4):
            down(4 * hh + i)
            if hh > 0:
                loop((F - 1) * i // 4, (F - 1) * (i + 1) // 4, lambda m: send_seq(hh - 1, m))
    loop(0, F - 1, lambda m: send_seq(HALVES - 1, m))

    for hh in range(HALVES):
        b_copy(hh, f).wait_recv()
        ybuf[0, 0:Q, :] = cbuf[hh, 1, f].astype(F32) + b_in[hh, f].astype(F32)

        def add_seq(i):
            p = peer(i)
            c_got(hh, p).wait_recv()
            ybuf[0, 0:Q, :] += c_in[hh, p].astype(F32)

        loop(1, F, add_seq)
        width = min(C, CH)
        for i in range(CH // width):
            at = hh * CH + i * width
            state = h_all[g * FG + at // C, slot(f), :, at % C:at % C + width].astype(F32)
            out_ref[:, at:at + width] = (state + ybuf[0, 0:Q, i * width:(i + 1) * width]).astype(BF16)

    def drain(i):
        rt_copy(i).wait_send()
        hs_copy(i).wait_send()
        for hh in range(HALVES):
            c_copy(hh, peer(i)).wait_send()

    loop(1, F, drain)

    def drain_h(i):
        for t in range(pieces):
            hz_copy(i, t).wait_send()

    loop(1, F, drain_h)

    @pl.when(own_part)
    def _():
        loop(1, F, lambda i: re_copy(i).wait_send())

    for e in (near, far, both):
        rs_copy(e).wait_send()

    def drain_all(k):
        for t in range(pieces):
            hx_copy(k, t).wait_send()
        hc_copy(k, 0).wait_send()
        hc_copy(k, 1).wait_send()
        for hh in range(HALVES):
            b_copy(hh, k).wait_send()

    loop(0, F, drain_all)
    for t in range(2):
        a_copy(HALVES - 1, t).wait_send()


def layer(F, G, queries, keys, values, out_weight, residual, norm_gain,
          route_ids, route_slots, route_weights, w_gate, w_up, w_down):
    Q = queries.shape[0]
    D = residual.shape[1]
    C = out_weight.shape[1]
    H = w_gate.shape[2]
    R = CAP * F
    FG = F // G
    C2 = D // G
    CH = C2 // HALVES
    gain = norm_gain.reshape(F, 1, C)
    vm = pl.BlockSpec(memory_space=pltpu.VMEM)
    hbm = pl.BlockSpec(memory_space=pltpu.HBM)
    dma = pltpu.SemaphoreType.DMA
    return pl.pallas_call(
        functools.partial(kernel, F, G),
        out_shape=jax.ShapeDtypeStruct((Q, C2), BF16),
        in_specs=[hbm] * 5 + [vm] * 4 + [hbm] * 3,
        out_specs=vm,
        scratch_shapes=[
            pltpu.VMEM(queries.shape, BF16),
            pltpu.VMEM(keys.shape[1:], BF16),
            pltpu.VMEM(values.shape[1:], BF16),
            pltpu.VMEM(out_weight.shape, BF16),
            pltpu.VMEM(residual.shape, BF16),
            pltpu.VMEM((F, Q, queries.shape[1]), BF16),
            pltpu.VMEM((F, 8, 128), jnp.int32),
            pltpu.VMEM((FG, Q, C), BF16),
            pltpu.VMEM((G, FG, Q, C), BF16),
            pltpu.VMEM((G, FG, Q, C), BF16),
            pltpu.VMEM((FG, Q, C), F32),
            pltpu.VMEM((F, F, Q, C), BF16),
            pltpu.VMEM((F, 2 * CAP, 128), F32),
            pltpu.VMEM((2, R, C), F32),
            pltpu.VMEM((2, R, 128), F32),
            pltpu.VMEM((2, 2, R, H), F32),
            pltpu.VMEM((2, R, H), BF16),
            pltpu.VMEM((2, R, CH), F32),
            pltpu.VMEM((2, F, Q, CH), BF16),
            pltpu.VMEM((HALVES, 2, F, Q, CH), BF16),
            pltpu.VMEM((HALVES, 2, F, Q, CH), BF16),
            pltpu.VMEM((HALVES, F, Q, CH), BF16),
            pltpu.VMEM((HALVES, F, Q, CH), BF16),
            pltpu.VMEM((2, 4, C, H), BF16),
            pltpu.VMEM((D_SLOTS, 2, H, CH), BF16),
            dma((5,)), dma((F,)), dma((F,)), dma((F,)), dma((F,)), dma((F,)), dma((FG,)),
            dma((G,)), dma((G,)), dma((F, 2)), dma((F, 2)), dma((F, 2)), dma((F, 2)),
            dma((F, 2)), dma((F, 2)), dma((HALVES, 2)), dma((HALVES, 2)), dma((HALVES, F)), dma((HALVES, F)),
            dma((HALVES, F)), dma((HALVES, F)), dma((2, 4)), dma((D_SLOTS, 2)),
        ],
        compiler_params=pltpu.CompilerParams(
            collective_id=0, has_side_effects=True, vmem_limit_bytes=VMEM),
    )(queries, keys[0], values[0], out_weight, residual, gain,
      route_ids.T, route_slots.T, route_weights.T, w_gate, w_up, w_down)


def solution(mesh):
    F, G = mesh.shape["fsdp"], mesh.shape["expert"]
    rows = P(("groups", "fsdp"), None)
    in_specs = (
        P(("groups", "fsdp"), "expert"),
        P(("groups", "fsdp"), None, "expert"),
        P(("groups", "fsdp"), None, "expert"),
        P("expert", "fsdp"),
        rows, P(), rows, rows, rows,
        P("expert", None, "fsdp"),
        P("expert", None, "fsdp"),
        P("expert", "fsdp", None),
    )
    return jax.shard_map(
        functools.partial(layer, F, G), mesh=mesh, in_specs=in_specs,
        out_specs=P(("groups", "fsdp"), "expert"), check_vma=False,
    )
```
